256 devices in a mesh: stem: 16 (over x, y_lo, core), grp: 16 (over z, y_hi).
Axes of the slice: x: 4, y: 4 (y_hi: 2, y_lo: 2; y = y_hi * 2 + y_lo), z: 8, core: 2. Of those that a mesh axis runs over, the one named last changes fastest.
Arguments:
- stem_tensor: float32 [256, 512, 512], P(None, 'stem', 'grp'), may hold values from -6 to 6
- left_factors: float32 [2, 16, 16, 256], P(None, 'grp'), may hold values from -0.375 to 0.375
- right_factors: float32 [2, 256, 1024], replicated, may hold values from -0.1875 to 0.1875
- index_labels: int32 [2, 9], replicated, may hold values from 0 to 8, each once within a row
Outputs:
- contracted: float32 [256, 512, 512], P(('stem', 'grp'))
The draws below stay inside these ranges and needn't reach their ends.
Inputs may be any that keep to these rules, and one draw needn't show every extreme that they name: `index_labels`: each row is a permutation of 0 to 8.
All inputs are finite; a program needn't handle non-finite values.
Results may differ from the reference program's by a relative error of at most 0.000098.
Values sent between devices are 32-bit elements; how exact they have to be, the bound alone decides.
A program may use at most 64 MiB of HBM per device.

```python
import jax
import jax.numpy as jnp
from jax import lax

BITS = 9
BOND = 256
SHARED = 512
HALF = 16
LOW = 32
OPEN = 256


def shard_levels(stream_key, extent, cuts, low, high):
    factor_of = 1.0
    for axis_at, shards_of in cuts:
        heights = jax.random.uniform(jax.random.fold_in(jax.random.fold_in(stream_key, 6), axis_at), (shards_of,), jnp.float32, low / len(cuts), high / len(cuts))
        factor_of = factor_of * jnp.repeat(jnp.exp(heights), extent[axis_at] // shards_of).reshape((-1,) + (1,) * (len(extent) - 1 - axis_at))
    return factor_of


def noise(own_key, dims, width, bound, shards=(), kind=jnp.bfloat16):
    entries = width * jax.random.normal(own_key, dims, jnp.float32)
    if shards:
        entries = entries * shard_levels(own_key, dims, shards, -0.22, 0.18)
    return jnp.clip(entries, -bound, bound).astype(kind)


def setup_inputs(seed: int = 0) -> dict:
    seeds = jax.random.split(jax.random.key(seed), 5)
    stem_tensor = noise(seeds[0], (OPEN, SHARED, SHARED), 1.0, 6.0, ((1, 16), (2, 16)), jnp.float32)
    left_factors = noise(seeds[1], (2, HALF, HALF, BOND), BOND ** -0.5, 0.375, ((1, 16),), jnp.float32)
    right_factors = noise(seeds[2], (2, BOND, LOW * LOW), (LOW * LOW) ** -0.5, 0.1875, (), jnp.float32)
    index_labels = jax.vmap(lambda own: jax.random.permutation(own, BITS))(jax.random.split(seeds[3], 2)).reshape((2, BITS)).astype(jnp.int32)
    return dict(stem_tensor=stem_tensor, left_factors=left_factors, right_factors=right_factors, index_labels=index_labels)


def build_branch(left, right, bit_order):
    upper = left.shape[0]
    table = right.reshape(right.shape[0], LOW, LOW)
    product = jnp.einsum('abk,kcd->acbd', left, table, precision=lax.Precision.HIGHEST)
    whole_branch = product.reshape(upper * LOW, upper * LOW)
    row_ids = jnp.arange(upper * LOW, dtype=jnp.int32)
    source_rows = jnp.zeros_like(row_ids)
    for bit_number in range(bit_order.shape[0]):
        picked = jnp.bitwise_and(jnp.right_shift(row_ids, bit_number), 1)
        source_rows = source_rows + jnp.left_shift(picked, bit_order[bit_number].astype(jnp.int32))
    return jnp.take(whole_branch, source_rows, axis=0)


def reference(stem_tensor, left_factors, right_factors, index_labels):
    branch_one = build_branch(left_factors[0], right_factors[0], index_labels[0])
    branch_two = build_branch(left_factors[1], right_factors[1], index_labels[1])

    def contract_slab(stem_block):
        halfway = jnp.dot(stem_block, branch_one, precision=lax.Precision.HIGHEST)
        return jnp.dot(halfway.T, branch_two, precision=lax.Precision.HIGHEST)

    return lax.map(contract_slab, stem_tensor)
```

```python
import jax
import jax.numpy as jnp
from jax import lax
from jax.experimental import pallas as pl
from jax.experimental.pallas import tpu as pltpu
from jax.sharding import PartitionSpec as P

MESH = pl.DeviceIdType.MESH
F32, BF16 = jnp.float32, jnp.bfloat16
OPEN, SHARED, BOND, LOW = 256, 512, 256, 32
CHUNKS = (0, 2, 1, 3)


def place():
    stem, grp = lax.axis_index("stem"), lax.axis_index("grp")
    return stem // 4, (stem // 2) % 2, stem % 2, grp // 2, grp % 2


def device(x, y_lo, core, z, y_hi):
    return x * 4 + y_lo * 2 + core, z * 2 + y_hi


def mesh_id(stem, grp):
    return {"stem": stem, "grp": grp}


def split(value):
    high = value.astype(BF16)
    return high, (value - high.astype(F32)).astype(BF16)


def swap_groups(a):
    lane = lax.broadcasted_iota(jnp.int32, a[0].shape, 1)
    low, even = lane < 64, (lane // 32) % 2 == 0

    def far(p, q):
        t = pltpu.roll(jnp.where(low, q, p), 64, 1)
        return jnp.where(low, p, t), jnp.where(low, t, q)

    def near(p, q):
        t = jnp.where(even, q, p)
        return jnp.where(even, p, pltpu.roll(t, 32, 1)), jnp.where(even, pltpu.roll(t, 96, 1), q)

    a0, a2 = far(a[0], a[2])
    a1, a3 = far(a[1], a[3])
    return near(a0, a1) + near(a2, a3)


def row_of(labels_ref, branch, index):
    source = jnp.zeros_like(index)
    for bit in range(9):
        picked = jnp.bitwise_and(jnp.right_shift(index, bit), 1)
        source = source + jnp.left_shift(picked, labels_ref[branch, bit])
    return jnp.bitwise_and(source, LOW - 1) * 16 + jnp.right_shift(source, 5)


def dot(a, b):
    return jnp.dot(a, b, preferred_element_type=F32)


def exchange(
    stem_hbm, left_hbm, right_hbm, labels_ref, acc_ref,
    stem_v, left_v, right_v, src, dst, piece, rows_in, rows_out, left_all,
    right_hi, right_lo, whole, b0_ref, b1_ref,
    load_sem, send_sem, recv_sem, row_send, row_recv, block_send, block_recv, y_sem, x_sem,
):
    x, y_lo, core, z, y_hi = place()
    stem, grp = lax.axis_index("stem"), lax.axis_index("grp")
    me = stem * 16 + grp
    y = y_hi * 2 + y_lo

    loads = [
        pltpu.make_async_copy(stem_hbm, stem_v, load_sem.at[0]),
        pltpu.make_async_copy(left_hbm, left_v, load_sem.at[1]),
        pltpu.make_async_copy(right_hbm, right_v, load_sem.at[2]),
    ]
    for load in loads:
        load.start()

    def column(k):
        return device(x, y_lo, core ^ (k // 8), lax.rem(z + (k * 3) % 8, 8), y_hi)

    def along_y(k):
        other = lax.rem(y + k, 4)
        return device(x, other % 2, core, z, other // 2)

    def along_x(k):
        return device(lax.rem(x + k, 4), y_lo, core, z, y_hi)

    barrier = pltpu.get_barrier_semaphore()

    @pl.loop(1, 16)
    def _(k):
        s, g = column(k)
        pl.semaphore_signal(barrier, inc=1, device_id=mesh_id(s, g), device_id_type=MESH)

    for k in range(1, 4):
        for s, g in (along_y(k), along_x(k)):
            pl.semaphore_signal(barrier, inc=1, device_id=mesh_id(s, g), device_id_type=MESH)

    loads[0].wait()
    for r in range(8):
        for half in range(2):
            lanes = slice(half * 128, half * 128 + 128)
            tall = jnp.concatenate([stem_v[a * 8 + r, :, lanes] for a in range(4)], axis=0)
            src[pl.ds(half * 1024 + r, 128, stride=8), :] = tall.T

    loads[1].wait()
    for b in range(2):
        row = left_v[b, pl.ds(stem, 1), :]
        for h in range(2):
            piece[b * 2 + h : b * 2 + h + 1, :] = row[:, h * 128 : h * 128 + 128]

    def slab(ref, index, count=1):
        return ref.at[pl.ds(pl.multiple_of(index * 8, 8), 8 * count), :]

    def send(s, g, dx):
        pltpu.make_async_remote_copy(
            src_ref=slab(src, s * 16 + g), dst_ref=slab(dst, me), send_sem=send_sem, recv_sem=recv_sem.at[dx],
            device_id=mesh_id(s, g), device_id_type=MESH,
        ).start()

    pl.semaphore_wait(barrier, 21)
    for k in range(1, 4):
        s, g = along_y(k)
        pl.semaphore_signal(y_sem, inc=1, device_id=mesh_id(s, g), device_id_type=MESH)

    @pl.loop(1, 16)
    def _(k):
        s, g = column(k)
        send(s, g, 0)

    pl.semaphore_wait(y_sem, 3)
    for k in range(1, 4):
        s, g = along_x(k)
        pl.semaphore_signal(x_sem, inc=1, device_id=mesh_id(s, g), device_id_type=MESH)

    @pl.loop(1, 16)
    def _(k):
        _, g = device(x, y_lo, core, lax.rem(z + (k * 3) % 8, 8), y_hi ^ (k // 8))
        pltpu.make_async_remote_copy(
            src_ref=piece, dst_ref=rows_in.at[grp], send_sem=row_send, recv_sem=row_recv,
            device_id=mesh_id(stem, g), device_id_type=MESH,
        ).start()

    def other(k, dx):
        return device(
            lax.rem(x + dx, 4), y_lo ^ (k // 8 % 2), core ^ (k // 16 % 2), lax.rem(z + (k * 3) % 8, 8), y_hi ^ (k // 32)
        )

    @pl.loop(0, 48)
    def _(n):
        q = n // 16 + 1
        s, g = device(x, y_lo ^ (q % 2), core ^ (n // 8 % 2), lax.rem(z + (n * 3) % 8, 8), y_hi ^ (q // 2))
        send(s, g, 0)

    slab_of_me = pl.ds(pl.multiple_of(me * 8, 8), 8)
    dst[slab_of_me, :] = src[slab_of_me, :]
    rows_in[pl.ds(grp, 1)] = piece[...][None]

    pl.semaphore_wait(x_sem, 3)

    rows15 = pltpu.make_async_remote_copy(
        src_ref=rows_in.at[pl.ds(0, 15)], dst_ref=rows_in.at[pl.ds(0, 15)], send_sem=row_send, recv_sem=row_recv,
        device_id=mesh_id(stem, grp), device_id_type=MESH,
    )
    rows15.wait_recv()
    for p in range(16):
        rows_out[p * 4 : p * 4 + 4, :] = rows_in[p]

    def block(s):
        return left_all.at[pl.ds(pl.multiple_of(s * 64, 64), 64), :]

    @pl.loop(1, 16)
    def _(k):
        s, _ = device(lax.rem(x + k // 4, 4), y_lo ^ (k // 2 % 2), core ^ (k % 2), z, y_hi)
        pltpu.make_async_remote_copy(
            src_ref=rows_out, dst_ref=block(stem), send_sem=block_send, recv_sem=block_recv,
            device_id=mesh_id(s, grp), device_id_type=MESH,
        ).start()

    left_all[pl.ds(pl.multiple_of(stem * 64, 64), 64), :] = rows_out[...]

    for dx in CHUNKS[1:]:
        @pl.loop(0, 64)
        def _(k):
            s, g = other(k, dx)
            send(s, g, dx)

    loads[2].wait()
    for b in range(2):
        right_hi[b], right_lo[b] = split(right_v[b])
    blocks15 = pltpu.make_async_remote_copy(
        src_ref=left_all.at[pl.ds(0, 960), :], dst_ref=left_all.at[pl.ds(0, 960), :], send_sem=block_send, recv_sem=block_recv,
        device_id=mesh_id(stem, grp), device_id_type=MESH,
    )
    blocks15.wait_recv()
    for b in range(2):
        left = jnp.concatenate([left_all[pl.ds(b * 2 + h, 256, stride=4), :] for h in range(2)], axis=1)
        left_hi, left_lo = split(left)
        for quad in range(8):
            lanes = slice(quad * 128, quad * 128 + 128)
            r_hi, r_lo = right_hi[b, :, lanes], right_lo[b, :, lanes]
            product = dot(left_hi, r_hi) + dot(left_hi, r_lo) + dot(left_lo, r_hi)
            for u4 in range(4):
                tiles = [product[(u4 * 4 + a) * 16 : (u4 * 4 + a) * 16 + 16, :] for a in range(4)]
                for q, tile in enumerate(swap_groups(tiles)):
                    whole[(quad * 4 + q) * 16 : (quad * 4 + q) * 16 + 16, u4 * 128 : u4 * 128 + 128] = tile
        if b == 0:
            index = lax.broadcasted_iota(jnp.int32, (1, SHARED), 1)
            here = lax.broadcasted_iota(jnp.int32, (SHARED, SHARED), 0)
            one_hot = jnp.where(here == row_of(labels_ref, b, index), 1.0, 0.0).astype(BF16)
            high, low = split(whole[...].T)
            b0_ref[0] = dot(high, one_hot).astype(BF16)
            b0_ref[1] = dot(low, one_hot).astype(BF16)
        else:
            index = lax.broadcasted_iota(jnp.int32, (SHARED, 1), 0)
            here = lax.broadcasted_iota(jnp.int32, (SHARED, SHARED), 1)
            one_hot = jnp.where(here == row_of(labels_ref, b, index), 1.0, 0.0).astype(BF16)
            high, low = split(whole[...])
            b1_ref[0] = dot(one_hot, high).astype(BF16)
            b1_ref[1] = dot(one_hot, low).astype(BF16)

    def nt(a, b):
        return lax.dot_general(a, b, (((1,), (1,)), ((), ())), preferred_element_type=F32)

    for number, dx in enumerate(CHUNKS):
        from_x = lax.rem(x + 4 - dx, 4)
        count = 63 if dx == 0 else 64
        pltpu.make_async_remote_copy(
            src_ref=slab(src, 0, count), dst_ref=slab(dst, 0, count), send_sem=send_sem, recv_sem=recv_sem.at[dx],
            device_id=mesh_id(stem, grp), device_id_type=MESH,
        ).wait_recv()
        rows = []
        for s in range(4):
            quads = []
            for g4 in range(4):
                tiles = []
                for h in range(4):
                    at = pl.multiple_of((from_x * 64 + s * 16 + g4 * 4 + h) * 8, 8)
                    tiles.append(dst[pl.ds(at, 8), :])
                quads.append(jnp.concatenate(swap_groups(tiles), axis=0))
            rows.append(jnp.concatenate(quads, axis=1))
        part_hi, part_lo = split(jnp.concatenate(rows, axis=0))
        half = nt(b0_ref[0], part_hi) + nt(b0_ref[0], part_lo) + nt(b0_ref[1], part_hi)
        half_hi, half_lo = split(half)
        at = pl.ds(pl.multiple_of(from_x * 128, 128), 128)
        c_hi, c_lo = b1_ref[0, at, :], b1_ref[1, at, :]
        term = dot(half_hi, c_hi) + dot(half_hi, c_lo) + dot(half_lo, c_hi)
        if number == 0:
            acc_ref[...] = term
        else:
            acc_ref[...] += term

    pltpu.make_async_remote_copy(
        src_ref=slab(src, 0, 255), dst_ref=slab(dst, 0, 255), send_sem=send_sem, recv_sem=recv_sem.at[0],
        device_id=mesh_id(stem, grp), device_id_type=MESH,
    ).wait_send()
    rows15.wait_send()
    blocks15.wait_send()


def write_out(acc_ref, out_ref, sem):
    copy = pltpu.make_async_copy(acc_ref, out_ref.at[0], sem)
    copy.start()
    copy.wait()


def on_device(stem_tensor, left_factors, right_factors, index_labels):
    hbm = pl.BlockSpec(memory_space=pltpu.HBM)
    dma = pltpu.SemaphoreType.DMA
    acc = pl.pallas_call(
        exchange,
        out_shape=jax.ShapeDtypeStruct((SHARED, SHARED), F32),
        in_specs=[hbm, hbm, hbm, pl.BlockSpec(memory_space=pltpu.SMEM)],
        out_specs=pl.BlockSpec(memory_space=pltpu.VMEM),
        scratch_shapes=[
            pltpu.VMEM((32, 32, 256), F32),
            pltpu.VMEM((2, 16, 256), F32),
            pltpu.VMEM((2, 256, 1024), F32),
            pltpu.VMEM((2048, 128), F32),
            pltpu.VMEM((2048, 128), F32),
            pltpu.VMEM((4, 128), F32),
            pltpu.VMEM((16, 4, 128), F32),
            pltpu.VMEM((64, 128), F32),
            pltpu.VMEM((1024, 128), F32),
            pltpu.VMEM((2, 256, 1024), BF16),
            pltpu.VMEM((2, 256, 1024), BF16),
            pltpu.VMEM((SHARED, SHARED), F32),
            pltpu.VMEM((2, SHARED, SHARED), BF16),
            pltpu.VMEM((2, SHARED, SHARED), BF16),
            dma((3,)), dma, dma((4,)), dma, dma, dma, dma,
            pltpu.SemaphoreType.REGULAR, pltpu.SemaphoreType.REGULAR,
        ],
        compiler_params=pltpu.CompilerParams(collective_id=0, has_side_effects=True, vmem_limit_bytes=40 * 1024 * 1024),
        name="exchange",
    )(jnp.transpose(stem_tensor, (1, 2, 0)), left_factors.reshape(2, 16, 256), right_factors, index_labels)
    return pl.pallas_call(
        write_out,
        out_shape=jax.ShapeDtypeStruct((1, SHARED, SHARED), F32),
        in_specs=[pl.BlockSpec(memory_space=pltpu.VMEM)],
        out_specs=hbm,
        scratch_shapes=[dma],
        compiler_params=pltpu.CompilerParams(vmem_limit_bytes=8 * 1024 * 1024),
        name="write_out",
    )(acc)


def solution(mesh):
    return jax.shard_map(
        on_device,
        mesh=mesh,
        in_specs=(P(None, "stem", "grp"), P(None, "grp", None, None), P(), P()),
        out_specs=P(("stem", "grp"), None, None),
        check_vma=False,
    )
```

```python
import jax
import jax.numpy as jnp
from jax import lax
from jax.experimental import pallas as pl
from jax.experimental.pallas import tpu as pltpu
from jax.sharding import PartitionSpec as P

MESH = pl.DeviceIdType.MESH
F32, BF16 = jnp.float32, jnp.bfloat16
OPEN, SHARED, BOND, LOW = 256, 512, 256, 32
CHUNKS = (0, 2, 1, 3)


def place():
    stem, grp = lax.axis_index("stem"), lax.axis_index("grp")
    return stem // 4, (stem // 2) % 2, stem % 2, grp // 2, grp % 2


def device(x, y_lo, core, z, y_hi):
    return x * 4 + y_lo * 2 + core, z * 2 + y_hi


def mesh_id(stem, grp):
    return {"stem": stem, "grp": grp}


def split(value):
    high = value.astype(BF16)
    return high, (value - high.astype(F32)).astype(BF16)


def swap_groups(a):
    lane = lax.broadcasted_iota(jnp.int32, a[0].shape, 1)
    low, even = lane < 64, (lane // 32) % 2 == 0

    def far(p, q):
        t = pltpu.roll(jnp.where(low, q, p), 64, 1)
        return jnp.where(low, p, t), jnp.where(low, t, q)

    def near(p, q):
        t = jnp.where(even, q, p)
        return jnp.where(even, p, pltpu.roll(t, 32, 1)), jnp.where(even, pltpu.roll(t, 96, 1), q)

    a0, a2 = far(a[0], a[2])
    a1, a3 = far(a[1], a[3])
    return near(a0, a1) + near(a2, a3)


def row_of(labels_ref, branch, index):
    source = jnp.zeros_like(index)
    for bit in range(9):
        picked = jnp.bitwise_and(jnp.right_shift(index, bit), 1)
        source = source + jnp.left_shift(picked, labels_ref[branch, bit])
    p = jnp.right_shift(source, 5)
    return jnp.bitwise_and(source, LOW - 1) * 16 + jnp.bitwise_and(p, 1) * 8 + jnp.right_shift(p, 1)


def dot(a, b):
    return jnp.dot(a, b, preferred_element_type=F32)


def exchange(
    stem_hbm, left_hbm, right_hbm, labels_hbm, acc_ref,
    labels_ref, stem_v, left_v, right_v, src, dst, piece, rows_in, rows_out, left_all,
    right_hi, right_lo, whole, one_hot, b0_ref, b1_ref,
    load_sem, send_sem, recv_sem, row_send, row_recv, block_send, block_recv, half_send, half_recv, y_sem, x_sem,
):
    x, y_lo, core, z, y_hi = place()
    stem, grp = lax.axis_index("stem"), lax.axis_index("grp")
    me = stem * 16 + grp
    y = y_hi * 2 + y_lo

    loads = [
        pltpu.make_async_copy(stem_hbm, stem_v, load_sem.at[0]),
        pltpu.make_async_copy(left_hbm, left_v, load_sem.at[1]),
        pltpu.make_async_copy(right_hbm, right_v, load_sem.at[2]),
        pltpu.make_async_copy(labels_hbm, labels_ref, load_sem.at[3]),
    ]
    for load in loads:
        load.start()

    def column(k):
        return device(x, y_lo, core ^ (k // 8), lax.rem(z + (k * 3) % 8, 8), y_hi)

    def along_y(k):
        other = lax.rem(y + k, 4)
        return device(x, other % 2, core, z, other // 2)

    def along_x(k):
        return device(lax.rem(x + k, 4), y_lo, core, z, y_hi)

    barrier = pltpu.get_barrier_semaphore()

    @pl.loop(1, 16)
    def _(k):
        s, g = column(k)
        pl.semaphore_signal(barrier, inc=1, device_id=mesh_id(s, g), device_id_type=MESH)

    for k in range(1, 4):
        for s, g in (along_y(k), along_x(k)):
            pl.semaphore_signal(barrier, inc=1, device_id=mesh_id(s, g), device_id_type=MESH)

    loads[0].wait()
    for r in range(8):
        for half in range(2):
            lanes = slice(half * 128, half * 128 + 128)
            tall = jnp.concatenate([stem_v[a * 8 + r, :, lanes] for a in range(4)], axis=0)
            src[pl.ds(half * 1024 + r, 128, stride=8), :] = tall.T

    loads[1].wait()
    for b in range(2):
        row = left_v[b, pl.ds(stem, 1), :]
        for h in range(2):
            piece[b * 2 + h : b * 2 + h + 1, :] = row[:, h * 128 : h * 128 + 128]

    def slab(ref, index, count=1):
        return ref.at[pl.ds(pl.multiple_of(index * 8, 8), 8 * count), :]

    def send(s, g, batch):
        pltpu.make_async_remote_copy(
            src_ref=slab(src, s * 16 + g), dst_ref=slab(dst, me), send_sem=send_sem, recv_sem=recv_sem.at[batch],
            device_id=mesh_id(s, g), device_id_type=MESH,
        ).start()

    def arrived(batch):
        count = 31 if batch == 0 else 32
        pltpu.make_async_remote_copy(
            src_ref=slab(src, 0, count), dst_ref=slab(dst, 0, count), send_sem=send_sem, recv_sem=recv_sem.at[batch],
            device_id=mesh_id(stem, grp), device_id_type=MESH,
        ).wait_recv()

    def issue(batch):
        group = batch // 2
        dx = CHUNKS[group]

        @pl.loop(batch % 2 * 32, batch % 2 * 32 + 32)
        def _(k):
            if group < 3:
                near, dz = k // 8, (k * 3) % 8
            else:
                near, far = k % 8, k // 8
                dz = jnp.where(far == 7, 0, jnp.where(far % 2 == 0, 4 - (far + 1) // 2, 4 + (far + 1) // 2))
            s, g = device(
                lax.rem(x + dx, 4), y_lo ^ (near % 2), core ^ (near // 2 % 2), lax.rem(z + dz, 8), 1 - y_hi ^ (near // 4)
            )
            send(s, g, batch)

    pl.semaphore_wait(barrier, 21)

    @pl.loop(1, 8)
    def _(k):
        s, g = device(x, y_lo, core, lax.rem(z + (k * 3) % 8, 8), y_hi)
        pltpu.make_async_remote_copy(
            src_ref=piece, dst_ref=rows_in.at[z], send_sem=row_send, recv_sem=row_recv,
            device_id=mesh_id(s, g), device_id_type=MESH,
        ).start()

    for k in (2, 1, 3):
        s, g = along_y(k)
        pl.semaphore_signal(y_sem.at[k], inc=1, device_id=mesh_id(s, g), device_id_type=MESH)

    @pl.loop(1, 16)
    def _(k):
        s, g = column(k)
        send(s, g, 0)

    def other_y(k, batch):
        to = lax.rem(y + k, 4)

        @pl.loop(0, 16)
        def _(n):
            s, g = device(x, to % 2, core ^ (n // 8), lax.rem(z + (n * 3) % 8, 8), to // 2)
            send(s, g, batch)

    pl.semaphore_wait(y_sem.at[3], 1)
    other_y(1, 0)
    pl.semaphore_wait(y_sem.at[1], 1)
    other_y(3, 1)
    pl.semaphore_wait(y_sem.at[2], 1)
    for k in (2, 1, 3):
        s, g = along_x(k)
        pl.semaphore_signal(x_sem.at[k], inc=1, device_id=mesh_id(s, g), device_id_type=MESH)
    other_y(2, 1)

    slab_of_me = pl.ds(pl.multiple_of(me * 8, 8), 8)
    dst[slab_of_me, :] = src[slab_of_me, :]
    rows_in[pl.ds(z, 1)] = piece[...][None]

    loads[2].wait()
    loads[3].wait()
    for b in range(2):
        right_hi[b], right_lo[b] = split(right_v[b])
        index = lax.broadcasted_iota(jnp.int32, (1, SHARED) if b == 0 else (SHARED, 1), 1 - b)
        here = lax.broadcasted_iota(jnp.int32, (SHARED, SHARED), b)
        one_hot[b] = jnp.where(here == row_of(labels_ref, b, index), 1.0, 0.0).astype(BF16)

    rows7 = pltpu.make_async_remote_copy(
        src_ref=rows_in.at[pl.ds(0, 7)], dst_ref=rows_in.at[pl.ds(0, 7)], send_sem=row_send, recv_sem=row_recv,
        device_id=mesh_id(stem, grp), device_id_type=MESH,
    )
    rows7.wait_recv()
    for p in range(8):
        rows_out[p * 4 : p * 4 + 4, :] = rows_in[p]
    for k in range(1, 4):
        pl.semaphore_wait(x_sem.at[k], 1)

    mine = left_all.at[pl.ds(pl.multiple_of((((core * 4 + x) * 2 + y_lo) * 2 + y_hi) * 32, 32), 32), :]

    @pl.loop(1, 16)
    def _(k):
        to = lax.rem(y + k % 4, 4)
        s, g = device(lax.rem(x + k // 4, 4), to % 2, core, z, to // 2)
        pltpu.make_async_remote_copy(
            src_ref=rows_out, dst_ref=mine, send_sem=block_send, recv_sem=block_recv,
            device_id=mesh_id(s, g), device_id_type=MESH,
        ).start()

    left_all[pl.ds(pl.multiple_of((((core * 4 + x) * 2 + y_lo) * 2 + y_hi) * 32, 32), 32), :] = rows_out[...]

    issue(2)
    issue(3)
    issue(4)
    issue(5)
    issue(6)
    issue(7)
    blocks15 = pltpu.make_async_remote_copy(
        src_ref=left_all.at[pl.ds(0, 480), :], dst_ref=left_all.at[pl.ds(0, 480), :], send_sem=block_send, recv_sem=block_recv,
        device_id=mesh_id(stem, grp), device_id_type=MESH,
    )
    blocks15.wait_recv()
    half_all = left_all.at[pl.ds(pl.multiple_of(core * 512, 512), 512), :]
    s, g = device(x, y_lo, 1 - core, z, y_hi)
    half_copy = pltpu.make_async_remote_copy(
        src_ref=half_all, dst_ref=half_all, send_sem=half_send, recv_sem=half_recv,
        device_id=mesh_id(s, g), device_id_type=MESH,
    )
    half_copy.start()
    half_copy.wait_recv()

    def assemble(b):
        left = jnp.concatenate([left_all[pl.ds(b * 2 + h, 256, stride=4), :] for h in range(2)], axis=1)
        left_hi, left_lo = split(left)
        for quad in range(8):
            lanes = slice(quad * 128, quad * 128 + 128)
            r_hi, r_lo = right_hi[b, :, lanes], right_lo[b, :, lanes]
            product = dot(left_hi, r_hi) + dot(left_hi, r_lo) + dot(left_lo, r_hi)
            for u4 in range(4):
                starts = [((a % 2) * 8 + u4 * 2 + a // 2) * 16 for a in range(4)]
                for q, tile in enumerate(swap_groups([product[at : at + 16, :] for at in starts])):
                    whole[(quad * 4 + q) * 16 : (quad * 4 + q) * 16 + 16, u4 * 128 : u4 * 128 + 128] = tile
        if b == 0:
            for part, value in enumerate(split(whole[...].T)):
                b0_ref[part] = dot(value, one_hot[b]).astype(BF16)
        else:
            for part, value in enumerate(split(whole[...])):
                b1_ref[part] = dot(one_hot[b], value).astype(BF16)

    def nt(a, b):
        return lax.dot_general(a, b, (((1,), (1,)), ((), ())), preferred_element_type=F32)

    def contract(number):
        from_x = lax.rem(x + 4 - CHUNKS[number], 4)
        rows = []
        for s in range(4):
            quads = []
            for g4 in range(4):
                tiles = []
                for h in range(4):
                    at = pl.multiple_of((from_x * 64 + s * 16 + g4 * 4 + h) * 8, 8)
                    tiles.append(dst[pl.ds(at, 8), :])
                quads.append(jnp.concatenate(swap_groups(tiles), axis=0))
            rows.append(jnp.concatenate(quads, axis=1))
        part_hi, part_lo = split(jnp.concatenate(rows, axis=0))
        half = nt(b0_ref[0], part_hi) + nt(b0_ref[0], part_lo) + nt(b0_ref[1], part_hi)
        half_hi, half_lo = split(half)
        at = pl.ds(pl.multiple_of(from_x * 128, 128), 128)
        c_hi, c_lo = b1_ref[0, at, :], b1_ref[1, at, :]
        term = dot(half_hi, c_hi) + dot(half_hi, c_lo) + dot(half_lo, c_hi)
        if number == 0:
            acc_ref[...] = term
        else:
            acc_ref[...] += term

    assemble(0)
    assemble(1)
    arrived(0)
    arrived(1)
    contract(0)
    arrived(2)
    arrived(3)
    contract(1)
    arrived(4)
    arrived(5)
    contract(2)
    arrived(6)
    arrived(7)
    contract(3)

    pltpu.make_async_remote_copy(
        src_ref=slab(src, 0, 255), dst_ref=slab(dst, 0, 255), send_sem=send_sem, recv_sem=recv_sem.at[0],
        device_id=mesh_id(stem, grp), device_id_type=MESH,
    ).wait_send()
    rows7.wait_send()
    blocks15.wait_send()
    half_copy.wait_send()


def write_out(acc_ref, out_ref, sem):
    copy = pltpu.make_async_copy(acc_ref, out_ref.at[0], sem)
    copy.start()
    copy.wait()


def on_device(stem_tensor, left_factors, right_factors, index_labels):
    hbm = pl.BlockSpec(memory_space=pltpu.HBM)
    dma = pltpu.SemaphoreType.DMA
    operands = jnp.transpose(stem_tensor, (1, 2, 0)), left_factors.reshape(2, 16, 256), right_factors, index_labels
    acc = pl.pallas_call(
        exchange,
        out_shape=jax.ShapeDtypeStruct((SHARED, SHARED), F32),
        in_specs=[hbm, hbm, hbm, hbm],
        out_specs=pl.BlockSpec(memory_space=pltpu.VMEM),
        scratch_shapes=[
            pltpu.SMEM((2, 9), jnp.int32),
            pltpu.VMEM((32, 32, 256), F32),
            pltpu.VMEM((2, 16, 256), F32),
            pltpu.VMEM((2, 256, 1024), F32),
            pltpu.VMEM((2048, 128), F32),
            pltpu.VMEM((2048, 128), F32),
            pltpu.VMEM((4, 128), F32),
            pltpu.VMEM((8, 4, 128), F32),
            pltpu.VMEM((32, 128), F32),
            pltpu.VMEM((1024, 128), F32),
            pltpu.VMEM((2, 256, 1024), BF16),
            pltpu.VMEM((2, 256, 1024), BF16),
            pltpu.VMEM((SHARED, SHARED), F32),
            pltpu.VMEM((2, SHARED, SHARED), BF16),
            pltpu.VMEM((2, SHARED, SHARED), BF16),
            pltpu.VMEM((2, SHARED, SHARED), BF16),
            dma((4,)), dma, dma((8,)), dma, dma, dma, dma, dma, dma,
            pltpu.SemaphoreType.REGULAR((4,)), pltpu.SemaphoreType.REGULAR((4,)),
        ],
        compiler_params=pltpu.CompilerParams(collective_id=0, has_side_effects=True, vmem_limit_bytes=40 * 1024 * 1024),
        name="exchange",
    )(*(pltpu.with_memory_space_constraint(a, pltpu.HBM) for a in operands))
    return pl.pallas_call(
        write_out,
        out_shape=jax.ShapeDtypeStruct((1, SHARED, SHARED), F32),
        in_specs=[pl.BlockSpec(memory_space=pltpu.VMEM)],
        out_specs=hbm,
        scratch_shapes=[dma],
        compiler_params=pltpu.CompilerParams(vmem_limit_bytes=8 * 1024 * 1024),
        name="write_out",
    )(acc)


def solution(mesh):
    return jax.shard_map(
        on_device,
        mesh=mesh,
        in_specs=(P(None, "stem", "grp"), P(None, "grp", None, None), P(), P()),
        out_specs=P(("stem", "grp"), None, None),
        check_vma=False,
    )
```

```python
import jax
import jax.numpy as jnp
from jax import lax
from jax.experimental import pallas as pl
from jax.experimental.pallas import tpu as pltpu
from jax.sharding import PartitionSpec as P

MESH = pl.DeviceIdType.MESH
F32, BF16 = jnp.float32, jnp.bfloat16
OPEN, SHARED, BOND, LOW = 256, 512, 256, 32
CHUNKS = (0, 2, 1, 3)


def place():
    stem, grp = lax.axis_index("stem"), lax.axis_index("grp")
    return stem // 4, (stem // 2) % 2, stem % 2, grp // 2, grp % 2


def device(x, y_lo, core, z, y_hi):
    return x * 4 + y_lo * 2 + core, z * 2 + y_hi


def mesh_id(stem, grp):
    return {"stem": stem, "grp": grp}


def split(value):
    high = value.astype(BF16)
    return high, (value - high.astype(F32)).astype(BF16)


def swap_groups(a):
    lane = lax.broadcasted_iota(jnp.int32, a[0].shape, 1)
    low, even = lane < 64, (lane // 32) % 2 == 0

    def far(p, q):
        t = pltpu.roll(jnp.where(low, q, p), 64, 1)
        return jnp.where(low, p, t), jnp.where(low, t, q)

    def near(p, q):
        t = jnp.where(even, q, p)
        return jnp.where(even, p, pltpu.roll(t, 32, 1)), jnp.where(even, pltpu.roll(t, 96, 1), q)

    a0, a2 = far(a[0], a[2])
    a1, a3 = far(a[1], a[3])
    return near(a0, a1) + near(a2, a3)


def row_of(labels_ref, branch, index):
    source = jnp.zeros_like(index)
    for bit in range(9):
        picked = jnp.bitwise_and(jnp.right_shift(index, bit), 1)
        source = source + jnp.left_shift(picked, labels_ref[branch, bit])
    p = jnp.right_shift(source, 5)
    return jnp.bitwise_and(source, LOW - 1) * 16 + jnp.bitwise_and(p, 1) * 8 + jnp.right_shift(p, 1)


def dot(a, b):
    return jnp.dot(a, b, preferred_element_type=F32)


def exchange(
    stem_hbm, left_hbm, right_hbm, labels_hbm, acc_ref,
    labels_ref, stem_v, left_v, right_v, src, dst, piece, rows_in, rows_out, left_all,
    right_hi, right_lo, whole, one_hot, b0_ref, b1_ref,
    load_sem, send_sem, recv_sem, row_send, row_recv, block_send, block_recv, half_send, half_recv, y_sem, x_sem,
):
    x, y_lo, core, z, y_hi = place()
    stem, grp = lax.axis_index("stem"), lax.axis_index("grp")
    me = stem * 16 + grp
    y = y_hi * 2 + y_lo

    loads = [
        pltpu.make_async_copy(stem_hbm, stem_v, load_sem.at[0]),
        pltpu.make_async_copy(left_hbm, left_v, load_sem.at[1]),
        pltpu.make_async_copy(right_hbm, right_v, load_sem.at[2]),
        pltpu.make_async_copy(labels_hbm, labels_ref, load_sem.at[3]),
    ]
    for load in loads:
        load.start()

    def column(k):
        return device(x, y_lo, core ^ (k // 8), lax.rem(z + (k * 3) % 8, 8), y_hi)

    def along_y(k):
        other = lax.rem(y + k, 4)
        return device(x, other % 2, core, z, other // 2)

    def along_x(k):
        return device(lax.rem(x + k, 4), y_lo, core, z, y_hi)

    barrier = pltpu.get_barrier_semaphore()

    @pl.loop(1, 16)
    def _(k):
        s, g = column(k)
        pl.semaphore_signal(barrier, inc=1, device_id=mesh_id(s, g), device_id_type=MESH)

    for k in range(1, 4):
        for s, g in (along_y(k), along_x(k)):
            pl.semaphore_signal(barrier, inc=1, device_id=mesh_id(s, g), device_id_type=MESH)

    loads[0].wait()
    for r in range(8):
        for half in range(2):
            lanes = slice(half * 128, half * 128 + 128)
            tall = jnp.concatenate([stem_v[a * 8 + r, :, lanes] for a in range(4)], axis=0)
            src[pl.ds(half * 1024 + r, 128, stride=8), :] = tall.T

    loads[1].wait()
    for b in range(2):
        row = left_v[b, pl.ds(stem, 1), :]
        for h in range(2):
            piece[b * 2 + h : b * 2 + h + 1, :] = row[:, h * 128 : h * 128 + 128]

    def slab(ref, index, count=1):
        return ref.at[pl.ds(pl.multiple_of(index * 8, 8), 8 * count), :]

    def send(s, g, batch):
        pltpu.make_async_remote_copy(
            src_ref=slab(src, s * 16 + g), dst_ref=slab(dst, me), send_sem=send_sem, recv_sem=recv_sem.at[batch],
            device_id=mesh_id(s, g), device_id_type=MESH,
        ).start()

    def arrived(batch):
        count = 31 if batch == 0 else 32
        pltpu.make_async_remote_copy(
            src_ref=slab(src, 0, count), dst_ref=slab(dst, 0, count), send_sem=send_sem, recv_sem=recv_sem.at[batch],
            device_id=mesh_id(stem, grp), device_id_type=MESH,
        ).wait_recv()

    def issue(batch):
        group = batch // 2
        dx = CHUNKS[group]

        @pl.loop(batch % 2 * 32, batch % 2 * 32 + 32)
        def _(k):
            near, dz = k // 8, (k * 3) % 8
            s, g = device(
                lax.rem(x + dx, 4), y_lo ^ (near % 2), core ^ (near // 2 % 2), lax.rem(z + dz, 8), 1 - y_hi ^ (near // 4)
            )
            send(s, g, batch)

    pl.semaphore_wait(barrier, 21)

    @pl.loop(1, 8)
    def _(k):
        s, g = device(x, y_lo, core, lax.rem(z + (k * 3) % 8, 8), y_hi)
        pltpu.make_async_remote_copy(
            src_ref=piece, dst_ref=rows_in.at[z], send_sem=row_send, recv_sem=row_recv,
            device_id=mesh_id(s, g), device_id_type=MESH,
        ).start()

    for k in (2, 1, 3):
        s, g = along_y(k)
        pl.semaphore_signal(y_sem.at[k], inc=1, device_id=mesh_id(s, g), device_id_type=MESH)

    @pl.loop(1, 16)
    def _(k):
        s, g = column(k)
        send(s, g, 0)

    def other_y(k, batch):
        to = lax.rem(y + k, 4)

        @pl.loop(0, 16)
        def _(n):
            s, g = device(x, to % 2, core ^ (n // 8), lax.rem(z + (n * 3) % 8, 8), to // 2)
            send(s, g, batch)

    pl.semaphore_wait(y_sem.at[3], 1)
    other_y(1, 0)
    pl.semaphore_wait(y_sem.at[1], 1)
    other_y(3, 1)
    pl.semaphore_wait(y_sem.at[2], 1)
    for k in (2, 1, 3):
        s, g = along_x(k)
        pl.semaphore_signal(x_sem.at[k], inc=1, device_id=mesh_id(s, g), device_id_type=MESH)
    other_y(2, 1)

    slab_of_me = pl.ds(pl.multiple_of(me * 8, 8), 8)
    dst[slab_of_me, :] = src[slab_of_me, :]
    rows_in[pl.ds(z, 1)] = piece[...][None]

    loads[2].wait()
    loads[3].wait()
    for b in range(2):
        right_hi[b], right_lo[b] = split(right_v[b])
        index = lax.broadcasted_iota(jnp.int32, (1, SHARED) if b == 0 else (SHARED, 1), 1 - b)
        here = lax.broadcasted_iota(jnp.int32, (SHARED, SHARED), b)
        one_hot[b] = jnp.where(here == row_of(labels_ref, b, index), 1.0, 0.0).astype(BF16)

    rows7 = pltpu.make_async_remote_copy(
        src_ref=rows_in.at[pl.ds(0, 7)], dst_ref=rows_in.at[pl.ds(0, 7)], send_sem=row_send, recv_sem=row_recv,
        device_id=mesh_id(stem, grp), device_id_type=MESH,
    )
    rows7.wait_recv()
    for p in range(8):
        rows_out[p * 4 : p * 4 + 4, :] = rows_in[p]
    for k in range(1, 4):
        pl.semaphore_wait(x_sem.at[k], 1)

    mine = left_all.at[pl.ds(pl.multiple_of((((core * 4 + x) * 2 + y_lo) * 2 + y_hi) * 32, 32), 32), :]

    @pl.loop(1, 16)
    def _(k):
        to = lax.rem(y + k % 4, 4)
        s, g = device(lax.rem(x + k // 4, 4), to % 2, core, z, to // 2)
        pltpu.make_async_remote_copy(
            src_ref=rows_out, dst_ref=mine, send_sem=block_send, recv_sem=block_recv,
            device_id=mesh_id(s, g), device_id_type=MESH,
        ).start()

    left_all[pl.ds(pl.multiple_of((((core * 4 + x) * 2 + y_lo) * 2 + y_hi) * 32, 32), 32), :] = rows_out[...]

    issue(2)
    issue(3)
    issue(4)
    issue(5)
    issue(6)
    issue(7)
    blocks15 = pltpu.make_async_remote_copy(
        src_ref=left_all.at[pl.ds(0, 480), :], dst_ref=left_all.at[pl.ds(0, 480), :], send_sem=block_send, recv_sem=block_recv,
        device_id=mesh_id(stem, grp), device_id_type=MESH,
    )
    blocks15.wait_recv()
    half_all = left_all.at[pl.ds(pl.multiple_of(core * 512, 512), 512), :]
    s, g = device(x, y_lo, 1 - core, z, y_hi)
    half_copy = pltpu.make_async_remote_copy(
        src_ref=half_all, dst_ref=half_all, send_sem=half_send, recv_sem=half_recv,
        device_id=mesh_id(s, g), device_id_type=MESH,
    )
    half_copy.start()
    half_copy.wait_recv()

    def assemble(b):
        left = jnp.concatenate([left_all[pl.ds(b * 2 + h, 256, stride=4), :] for h in range(2)], axis=1)
        left_hi, left_lo = split(left)
        left_all_parts = jnp.concatenate([left_hi, left_hi, left_lo], axis=1)
        for quad in range(8):
            lanes = slice(quad * 128, quad * 128 + 128)
            r_hi, r_lo = right_hi[b, :, lanes], right_lo[b, :, lanes]
            product = dot(left_all_parts, jnp.concatenate([r_hi, r_lo, r_hi], axis=0))
            for u4 in range(4):
                starts = [((a % 2) * 8 + u4 * 2 + a // 2) * 16 for a in range(4)]
                for q, tile in enumerate(swap_groups([product[at : at + 16, :] for at in starts])):
                    whole[(quad * 4 + q) * 16 : (quad * 4 + q) * 16 + 16, u4 * 128 : u4 * 128 + 128] = tile
        if b == 0:
            for part, value in enumerate(split(whole[...].T)):
                b0_ref[part] = dot(value, one_hot[b]).astype(BF16)
        else:
            for part, value in enumerate(split(whole[...])):
                b1_ref[part] = dot(one_hot[b], value).astype(BF16)

    def nt(a, b):
        return lax.dot_general(a, b, (((1,), (1,)), ((), ())), preferred_element_type=F32)

    def contract(number):
        from_x = lax.rem(x + 4 - CHUNKS[number], 4)
        rows = []
        for s in range(4):
            quads = []
            for g4 in range(4):
                tiles = []
                for h in range(4):
                    at = pl.multiple_of((from_x * 64 + s * 16 + g4 * 4 + h) * 8, 8)
                    tiles.append(dst[pl.ds(at, 8), :])
                quads.append(jnp.concatenate(swap_groups(tiles), axis=0))
            rows.append(jnp.concatenate(quads, axis=1))
        part_hi, part_lo = split(jnp.concatenate(rows, axis=0))
        half = nt(
            jnp.concatenate([b0_ref[0], b0_ref[0], b0_ref[1]], axis=1),
            jnp.concatenate([part_hi, part_lo, part_hi], axis=1),
        )
        half_hi, half_lo = split(half)
        at = pl.ds(pl.multiple_of(from_x * 128, 128), 128)
        c_hi, c_lo = b1_ref[0, at, :], b1_ref[1, at, :]
        term = dot(
            jnp.concatenate([half_hi, half_hi, half_lo], axis=1),
            jnp.concatenate([c_hi, c_lo, c_hi], axis=0),
        )
        if number == 0:
            acc_ref[...] = term
        else:
            acc_ref[...] += term

    assemble(0)
    assemble(1)
    arrived(0)
    arrived(1)
    contract(0)
    arrived(2)
    arrived(3)
    contract(1)
    arrived(4)
    arrived(5)
    contract(2)
    arrived(6)
    arrived(7)
    contract(3)

    pltpu.make_async_remote_copy(
        src_ref=slab(src, 0, 255), dst_ref=slab(dst, 0, 255), send_sem=send_sem, recv_sem=recv_sem.at[0],
        device_id=mesh_id(stem, grp), device_id_type=MESH,
    ).wait_send()
    rows7.wait_send()
    blocks15.wait_send()
    half_copy.wait_send()


def write_out(acc_ref, out_ref, sem):
    copy = pltpu.make_async_copy(acc_ref, out_ref.at[0], sem)
    copy.start()
    copy.wait()


def on_device(stem_tensor, left_factors, right_factors, index_labels):
    hbm = pl.BlockSpec(memory_space=pltpu.HBM)
    dma = pltpu.SemaphoreType.DMA
    operands = jnp.transpose(stem_tensor, (1, 2, 0)), left_factors.reshape(2, 16, 256), right_factors, index_labels
    acc = pl.pallas_call(
        exchange,
        out_shape=jax.ShapeDtypeStruct((SHARED, SHARED), F32),
        in_specs=[hbm, hbm, hbm, hbm],
        out_specs=pl.BlockSpec(memory_space=pltpu.VMEM),
        scratch_shapes=[
            pltpu.SMEM((2, 9), jnp.int32),
            pltpu.VMEM((32, 32, 256), F32),
            pltpu.VMEM((2, 16, 256), F32),
            pltpu.VMEM((2, 256, 1024), F32),
            pltpu.VMEM((2048, 128), F32),
            pltpu.VMEM((2048, 128), F32),
            pltpu.VMEM((4, 128), F32),
            pltpu.VMEM((8, 4, 128), F32),
            pltpu.VMEM((32, 128), F32),
            pltpu.VMEM((1024, 128), F32),
            pltpu.VMEM((2, 256, 1024), BF16),
            pltpu.VMEM((2, 256, 1024), BF16),
            pltpu.VMEM((SHARED, SHARED), F32),
            pltpu.VMEM((2, SHARED, SHARED), BF16),
            pltpu.VMEM((2, SHARED, SHARED), BF16),
            pltpu.VMEM((2, SHARED, SHARED), BF16),
            dma((4,)), dma, dma((8,)), dma, dma, dma, dma, dma, dma,
            pltpu.SemaphoreType.REGULAR((4,)), pltpu.SemaphoreType.REGULAR((4,)),
        ],
        compiler_params=pltpu.CompilerParams(collective_id=0, has_side_effects=True, vmem_limit_bytes=40 * 1024 * 1024),
        name="exchange",
    )(*(pltpu.with_memory_space_constraint(a, pltpu.HBM) for a in operands))
    return pl.pallas_call(
        write_out,
        out_shape=jax.ShapeDtypeStruct((1, SHARED, SHARED), F32),
        in_specs=[pl.BlockSpec(memory_space=pltpu.VMEM)],
        out_specs=hbm,
        scratch_shapes=[dma],
        compiler_params=pltpu.CompilerParams(vmem_limit_bytes=8 * 1024 * 1024),
        name="write_out",
    )(acc)


def solution(mesh):
    return jax.shard_map(
        on_device,
        mesh=mesh,
        in_specs=(P(None, "stem", "grp"), P(None, "grp", None, None), P(), P()),
        out_specs=P(("stem", "grp"), None, None),
        check_vma=False,
    )
```

```python
import jax
import jax.numpy as jnp
from jax import lax
from jax.experimental import pallas as pl
from jax.experimental.pallas import tpu as pltpu
from jax.sharding import PartitionSpec as P

MESH = pl.DeviceIdType.MESH
F32, BF16 = jnp.float32, jnp.bfloat16
OPEN, SHARED, BOND, LOW = 256, 512, 256, 32
CHUNKS = (0, 2, 1, 3)


def place():
    stem, grp = lax.axis_index("stem"), lax.axis_index("grp")
    return stem // 4, (stem // 2) % 2, stem % 2, grp // 2, grp % 2


def device(x, y_lo, core, z, y_hi):
    return x * 4 + y_lo * 2 + core, z * 2 + y_hi


def mesh_id(stem, grp):
    return {"stem": stem, "grp": grp}


def split(value):
    high = value.astype(BF16)
    return high, (value - high.astype(F32)).astype(BF16)


def swap_groups(a):
    lane = lax.broadcasted_iota(jnp.int32, a[0].shape, 1)
    low, even = lane < 64, (lane // 32) % 2 == 0

    def far(p, q):
        t = pltpu.roll(jnp.where(low, q, p), 64, 1)
        return jnp.where(low, p, t), jnp.where(low, t, q)

    def near(p, q):
        t = jnp.where(even, q, p)
        return jnp.where(even, p, pltpu.roll(t, 32, 1)), jnp.where(even, pltpu.roll(t, 96, 1), q)

    a0, a2 = far(a[0], a[2])
    a1, a3 = far(a[1], a[3])
    return near(a0, a1) + near(a2, a3)


def row_of(labels_ref, branch, index):
    source = jnp.zeros_like(index)
    for bit in range(9):
        picked = jnp.bitwise_and(jnp.right_shift(index, bit), 1)
        source = source + jnp.left_shift(picked, labels_ref[branch, bit])
    p = jnp.right_shift(source, 5)
    return jnp.bitwise_and(source, LOW - 1) * 16 + jnp.bitwise_and(p, 1) * 8 + jnp.right_shift(p, 1)


def dot(a, b):
    return jnp.dot(a, b, preferred_element_type=F32)


def exchange(
    stem_hbm, left_hbm, right_hbm, labels_hbm, acc_ref,
    labels_ref, stem_v, left_v, right_v, src, dst, piece, rows_in, rows_out, left_all,
    right_hi, right_lo, whole, one_hot, b0_ref, b1_ref,
    load_sem, send_sem, recv_sem, row_send, row_recv, block_send, block_recv, half_send, half_recv, y_sem, x_sem,
):
    x, y_lo, core, z, y_hi = place()
    stem, grp = lax.axis_index("stem"), lax.axis_index("grp")
    me = stem * 16 + grp
    y = y_hi * 2 + y_lo

    loads = [
        pltpu.make_async_copy(stem_hbm, stem_v, load_sem.at[0]),
        pltpu.make_async_copy(left_hbm, left_v, load_sem.at[1]),
        pltpu.make_async_copy(right_hbm, right_v, load_sem.at[2]),
        pltpu.make_async_copy(labels_hbm, labels_ref, load_sem.at[3]),
    ]
    for load in loads:
        load.start()

    def column(k):
        return device(x, y_lo, core ^ (k // 8), lax.rem(z + (k * 3) % 8, 8), y_hi)

    def along_y(k):
        other = lax.rem(y + k, 4)
        return device(x, other % 2, core, z, other // 2)

    def along_x(k):
        return device(lax.rem(x + k, 4), y_lo, core, z, y_hi)

    barrier = pltpu.get_barrier_semaphore()

    @pl.loop(1, 16)
    def _(k):
        s, g = column(k)
        pl.semaphore_signal(barrier, inc=1, device_id=mesh_id(s, g), device_id_type=MESH)

    for k in range(1, 4):
        for s, g in (along_y(k), along_x(k)):
            pl.semaphore_signal(barrier, inc=1, device_id=mesh_id(s, g), device_id_type=MESH)

    loads[0].wait()
    for r in range(8):
        for half in range(2):
            lanes = slice(half * 128, half * 128 + 128)
            tall = jnp.concatenate([stem_v[a * 8 + r, :, lanes] for a in range(4)], axis=0)
            src[pl.ds(half * 1024 + r, 128, stride=8), :] = tall.T

    loads[1].wait()
    for b in range(2):
        row = left_v[b, pl.ds(stem, 1), :]
        for h in range(2):
            piece[b * 2 + h : b * 2 + h + 1, :] = row[:, h * 128 : h * 128 + 128]

    def slab(ref, index, count=1):
        return ref.at[pl.ds(pl.multiple_of(index * 8, 8), 8 * count), :]

    def send(s, g, batch):
        pltpu.make_async_remote_copy(
            src_ref=slab(src, s * 16 + g), dst_ref=slab(dst, me), send_sem=send_sem, recv_sem=recv_sem.at[batch],
            device_id=mesh_id(s, g), device_id_type=MESH,
        ).start()

    def arrived(batch):
        count = 31 if batch == 0 else 32
        pltpu.make_async_remote_copy(
            src_ref=slab(src, 0, count), dst_ref=slab(dst, 0, count), send_sem=send_sem, recv_sem=recv_sem.at[batch],
            device_id=mesh_id(stem, grp), device_id_type=MESH,
        ).wait_recv()

    def issue(batch):
        group = batch // 2
        dx = CHUNKS[group]

        @pl.loop(batch % 2 * 32, batch % 2 * 32 + 32)
        def _(k):
            near, dz = k // 8, (k * 3) % 8
            s, g = device(
                lax.rem(x + dx, 4), y_lo ^ (near % 2), core ^ (near // 2 % 2), lax.rem(z + dz, 8), 1 - y_hi ^ (near // 4)
            )
            send(s, g, batch)

    pl.semaphore_wait(barrier, 21)

    @pl.loop(1, 8)
    def _(k):
        s, g = device(x, y_lo, core, lax.rem(z + (k * 3) % 8, 8), y_hi)
        pltpu.make_async_remote_copy(
            src_ref=piece, dst_ref=rows_in.at[z], send_sem=row_send, recv_sem=row_recv,
            device_id=mesh_id(s, g), device_id_type=MESH,
        ).start()

    for k in (2, 1, 3):
        s, g = along_y(k)
        pl.semaphore_signal(y_sem.at[k], inc=1, device_id=mesh_id(s, g), device_id_type=MESH)

    @pl.loop(1, 16)
    def _(k):
        s, g = column(k)
        send(s, g, 0)

    def other_y(k, batch):
        to = lax.rem(y + k, 4)

        @pl.loop(0, 16)
        def _(n):
            s, g = device(x, to % 2, core ^ (n // 8), lax.rem(z + (n * 3) % 8, 8), to // 2)
            send(s, g, batch)

    pl.semaphore_wait(y_sem.at[3], 1)
    other_y(1, 0)
    pl.semaphore_wait(y_sem.at[1], 1)
    other_y(3, 1)
    pl.semaphore_wait(y_sem.at[2], 1)
    for k in (2, 1, 3):
        s, g = along_x(k)
        pl.semaphore_signal(x_sem.at[k], inc=1, device_id=mesh_id(s, g), device_id_type=MESH)
    other_y(2, 1)

    slab_of_me = pl.ds(pl.multiple_of(me * 8, 8), 8)
    dst[slab_of_me, :] = src[slab_of_me, :]
    rows_in[pl.ds(z, 1)] = piece[...][None]

    rows7 = pltpu.make_async_remote_copy(
        src_ref=rows_in.at[pl.ds(0, 7)], dst_ref=rows_in.at[pl.ds(0, 7)], send_sem=row_send, recv_sem=row_recv,
        device_id=mesh_id(stem, grp), device_id_type=MESH,
    )
    rows7.wait_recv()
    for p in range(8):
        rows_out[p * 4 : p * 4 + 4, :] = rows_in[p]
    for k in range(1, 4):
        pl.semaphore_wait(x_sem.at[k], 1)

    mine = left_all.at[pl.ds(pl.multiple_of((((core * 4 + x) * 2 + y_lo) * 2 + y_hi) * 32, 32), 32), :]

    @pl.loop(1, 16)
    def _(k):
        to = lax.rem(y + k % 4, 4)
        s, g = device(lax.rem(x + k // 4, 4), to % 2, core, z, to // 2)
        pltpu.make_async_remote_copy(
            src_ref=rows_out, dst_ref=mine, send_sem=block_send, recv_sem=block_recv,
            device_id=mesh_id(s, g), device_id_type=MESH,
        ).start()

    left_all[pl.ds(pl.multiple_of((((core * 4 + x) * 2 + y_lo) * 2 + y_hi) * 32, 32), 32), :] = rows_out[...]

    issue(2)
    issue(3)
    issue(4)
    issue(5)
    issue(6)
    issue(7)
    loads[2].wait()
    loads[3].wait()
    for b in range(2):
        right_hi[b], right_lo[b] = split(right_v[b])
        index = lax.broadcasted_iota(jnp.int32, (1, SHARED) if b == 0 else (SHARED, 1), 1 - b)
        here = lax.broadcasted_iota(jnp.int32, (SHARED, SHARED), b)
        one_hot[b] = jnp.where(here == row_of(labels_ref, b, index), 1.0, 0.0).astype(BF16)

    blocks15 = pltpu.make_async_remote_copy(
        src_ref=left_all.at[pl.ds(0, 480), :], dst_ref=left_all.at[pl.ds(0, 480), :], send_sem=block_send, recv_sem=block_recv,
        device_id=mesh_id(stem, grp), device_id_type=MESH,
    )
    blocks15.wait_recv()
    half_all = left_all.at[pl.ds(pl.multiple_of(core * 512, 512), 512), :]
    s, g = device(x, y_lo, 1 - core, z, y_hi)
    half_copy = pltpu.make_async_remote_copy(
        src_ref=half_all, dst_ref=half_all, send_sem=half_send, recv_sem=half_recv,
        device_id=mesh_id(s, g), device_id_type=MESH,
    )
    half_copy.start()
    half_copy.wait_recv()

    def assemble(b):
        left = jnp.concatenate([left_all[pl.ds(b * 2 + h, 256, stride=4), :] for h in range(2)], axis=1)
        left_hi, left_lo = split(left)
        left_all_parts = jnp.concatenate([left_hi, left_hi, left_lo], axis=1)
        for quad in range(8):
            lanes = slice(quad * 128, quad * 128 + 128)
            r_hi, r_lo = right_hi[b, :, lanes], right_lo[b, :, lanes]
            product = dot(left_all_parts, jnp.concatenate([r_hi, r_lo, r_hi], axis=0))
            for u4 in range(4):
                starts = [((a % 2) * 8 + u4 * 2 + a // 2) * 16 for a in range(4)]
                for q, tile in enumerate(swap_groups([product[at : at + 16, :] for at in starts])):
                    whole[(quad * 4 + q) * 16 : (quad * 4 + q) * 16 + 16, u4 * 128 : u4 * 128 + 128] = tile
        if b == 0:
            for part, value in enumerate(split(whole[...].T)):
                b0_ref[part] = dot(value, one_hot[b]).astype(BF16)
        else:
            for part, value in enumerate(split(whole[...])):
                b1_ref[part] = dot(one_hot[b], value).astype(BF16)

    def nt(a, b):
        return lax.dot_general(a, b, (((1,), (1,)), ((), ())), preferred_element_type=F32)

    def contract(number):
        from_x = lax.rem(x + 4 - CHUNKS[number], 4)
        rows = []
        for s in range(4):
            quads = []
            for g4 in range(4):
                tiles = []
                for h in range(4):
                    at = pl.multiple_of((from_x * 64 + s * 16 + g4 * 4 + h) * 8, 8)
                    tiles.append(dst[pl.ds(at, 8), :])
                quads.append(jnp.concatenate(swap_groups(tiles), axis=0))
            rows.append(jnp.concatenate(quads, axis=1))
        part_hi, part_lo = split(jnp.concatenate(rows, axis=0))
        half = nt(
            jnp.concatenate([b0_ref[0], b0_ref[0], b0_ref[1]], axis=1),
            jnp.concatenate([part_hi, part_lo, part_hi], axis=1),
        )
        half_hi, half_lo = split(half)
        at = pl.ds(pl.multiple_of(from_x * 128, 128), 128)
        c_hi, c_lo = b1_ref[0, at, :], b1_ref[1, at, :]
        term = dot(
            jnp.concatenate([half_hi, half_hi, half_lo], axis=1),
            jnp.concatenate([c_hi, c_lo, c_hi], axis=0),
        )
        if number == 0:
            acc_ref[...] = term
        else:
            acc_ref[...] += term

    assemble(0)
    assemble(1)
    arrived(0)
    arrived(1)
    contract(0)
    arrived(2)
    arrived(3)
    contract(1)
    arrived(4)
    arrived(5)
    contract(2)
    arrived(6)
    arrived(7)
    contract(3)

    pltpu.make_async_remote_copy(
        src_ref=slab(src, 0, 255), dst_ref=slab(dst, 0, 255), send_sem=send_sem, recv_sem=recv_sem.at[0],
        device_id=mesh_id(stem, grp), device_id_type=MESH,
    ).wait_send()
    rows7.wait_send()
    blocks15.wait_send()
    half_copy.wait_send()


def write_out(acc_ref, out_ref, sem):
    copy = pltpu.make_async_copy(acc_ref, out_ref.at[0], sem)
    copy.start()
    copy.wait()


def on_device(stem_tensor, left_factors, right_factors, index_labels):
    hbm = pl.BlockSpec(memory_space=pltpu.HBM)
    dma = pltpu.SemaphoreType.DMA
    operands = jnp.transpose(stem_tensor, (1, 2, 0)), left_factors.reshape(2, 16, 256), right_factors, index_labels
    acc = pl.pallas_call(
        exchange,
        out_shape=jax.ShapeDtypeStruct((SHARED, SHARED), F32),
        in_specs=[hbm, hbm, hbm, hbm],
        out_specs=pl.BlockSpec(memory_space=pltpu.VMEM),
        scratch_shapes=[
            pltpu.SMEM((2, 9), jnp.int32),
            pltpu.VMEM((32, 32, 256), F32),
            pltpu.VMEM((2, 16, 256), F32),
            pltpu.VMEM((2, 256, 1024), F32),
            pltpu.VMEM((2048, 128), F32),
            pltpu.VMEM((2048, 128), F32),
            pltpu.VMEM((4, 128), F32),
            pltpu.VMEM((8, 4, 128), F32),
            pltpu.VMEM((32, 128), F32),
            pltpu.VMEM((1024, 128), F32),
            pltpu.VMEM((2, 256, 1024), BF16),
            pltpu.VMEM((2, 256, 1024), BF16),
            pltpu.VMEM((SHARED, SHARED), F32),
            pltpu.VMEM((2, SHARED, SHARED), BF16),
            pltpu.VMEM((2, SHARED, SHARED), BF16),
            pltpu.VMEM((2, SHARED, SHARED), BF16),
            dma((4,)), dma, dma((8,)), dma, dma, dma, dma, dma, dma,
            pltpu.SemaphoreType.REGULAR((4,)), pltpu.SemaphoreType.REGULAR((4,)),
        ],
        compiler_params=pltpu.CompilerParams(collective_id=0, has_side_effects=True, vmem_limit_bytes=40 * 1024 * 1024),
        name="exchange",
    )(*(pltpu.with_memory_space_constraint(a, pltpu.HBM) for a in operands))
    return pl.pallas_call(
        write_out,
        out_shape=jax.ShapeDtypeStruct((1, SHARED, SHARED), F32),
        in_specs=[pl.BlockSpec(memory_space=pltpu.VMEM)],
        out_specs=hbm,
        scratch_shapes=[dma],
        compiler_params=pltpu.CompilerParams(vmem_limit_bytes=8 * 1024 * 1024),
        name="write_out",
    )(acc)


def solution(mesh):
    return jax.shard_map(
        on_device,
        mesh=mesh,
        in_specs=(P(None, "stem", "grp"), P(None, "grp", None, None), P(), P()),
        out_specs=P(("stem", "grp"), None, None),
        check_vma=False,
    )
```
